32 devices in a mesh: dp: 2 (over y), ep: 16 (over z, x, core).
Axes of the slice: x: 2, y: 2, z: 4, core: 2. Of those that a mesh axis runs over, the one named last changes fastest.
Arguments:
- tokens: bfloat16 [3072, 2048], P(('dp', 'ep')), parts along dimension 0, may hold values from -6 to 6
- routes: int32 [3072, 8], P(('dp', 'ep')), parts along dimension 0, may hold values from 0 to 15, all different within a row; in each aligned block of 96 rows (0 to 95, 96 to 191, ...) at most 72 rows name the same one
- combine_weights: bfloat16 [3072, 8], P(('dp', 'ep')), parts along dimension 0, may hold values from 0.049804688 to 1
- w_gate: bfloat16 [16, 2048, 768], P('ep'), may hold values from -0.125 to 0.125
- w_up: bfloat16 [16, 2048, 768], P('ep'), may hold values from -0.125 to 0.125
- w_down: bfloat16 [16, 768, 2048], P('ep'), may hold values from -0.21875 to 0.21875
Outputs:
- mixed: bfloat16 [3072, 2048], P(('dp', 'ep')), parts along dimension 0
The draws below stay inside these ranges and needn't reach their ends.
There are 2 independent parts, one for each index of `dp`. The reference program is written for one: setup_inputs(seed, part) draws one part's arguments, and reference() takes and returns one part's arrays. A program takes and returns all parts, laid end to end along the dimension named above; an argument that names none is the same for every part. Nothing has to cross between parts.
Inputs may be any that keep to these rules, and one draw needn't show every extreme that they name: `routes`: each row names 8 different experts. Among the 96 rows of one device no expert is named by more than 72 rows, a bound that some blocks reach.
All inputs are finite; a program needn't handle non-finite values.
Results may differ from the reference program's by a relative error of at most 0.012.
Values may be sent and summed in bfloat16 or wider, within the bound.
No kernel may reach another device: no remote copies, remote signals or barrier semaphores. Data moves between devices by JAX's collectives and lax.ppermute only.
A program may use at most 128 MiB of HBM per device.

```python
import math
import jax
import jax.numpy as jnp
import numpy as np
from jax import lax

D = 2048
FF = 768
TOP = 8
TOK_DEV = 96
EXPERTS = 16
CAP = 72
TOKENS = 1536
N_EP = 16


def shard_levels(key, extent, cuts, smallest, high):
    gain = 1.0
    for dim, shards_of in cuts:
        steps = jax.random.uniform(jax.random.fold_in(jax.random.fold_in(key, 6), dim), (shards_of,), jnp.float32, smallest / len(cuts), high / len(cuts))
        gain = gain * jnp.repeat(jnp.exp(steps), extent[dim] // shards_of).reshape((-1,) + (1,) * (len(extent) - 1 - dim))
    return gain


def routed_block(rng, own, number, rows, count, top, bound, skew):
    ranking = jax.random.permutation(rng, count)
    crowded, ordinary = load_shares(count, rows * top, bound, skew, True), load_shares(count, rows * top, bound, skew, False)
    places = jnp.arange(count)

    def named(tallies, turn):
        used = int((tallies > 0).sum())
        fixed = max(1, used // 4)
        moved = fixed + (places - fixed + turn * (used - fixed)) % max(1, count - fixed)
        return jnp.zeros((count,), jnp.int32).at[ranking[jnp.where(places < fixed, places, moved)]].set(jnp.asarray(tallies, jnp.int32))

    tallies = jnp.where(number % 4 == 0, named(crowded, number // 4), named(ordinary, number - number // 4 - 1))
    mixed = jax.random.permutation(jax.random.fold_in(own, 3), count)
    source_of, sink = mixed[0:count // 2 * 2:2], mixed[1:count // 2 * 2:2]
    slack = jnp.minimum(tallies[source_of] - 1, bound - tallies[sink]) // 2
    slack = jnp.where((source_of == ranking[0]) | (sink == ranking[0]) | (tallies[sink] == 0), 0, jnp.maximum(slack, 0))
    moved = jax.random.randint(jax.random.fold_in(own, 4), (count // 2,), 0, 1 << 20) % (slack + 1)
    tallies = tallies.at[source_of].add(-moved).at[sink].add(moved)
    members = jnp.searchsorted(jnp.cumsum(tallies), jnp.arange(rows * top), side="right").astype(jnp.int32)
    listing = members.reshape(top, rows).T
    listing = listing[jax.random.permutation(jax.random.fold_in(own, 1), rows)]
    turn = jax.random.randint(jax.random.fold_in(own, 2), (rows, 1), 0, top)
    return jnp.take_along_axis(listing, (jnp.arange(top)[None, :] + turn) % top, axis=1)


def load_shares(number_of, total, reach, skew, full):
    loads = [(1 << 20) // math.isqrt(grade ** skew) + 1 for grade in range(1, number_of + 1)]
    largest = reach if full else min(reach, max(-(-total // number_of), total * loads[0] // sum(loads)))
    least = 1 if total - largest >= number_of - 1 else 0
    given, spare = [largest] + [least] * (number_of - 1), total - largest - least * (number_of - 1)
    while spare > 0:
        candidates = [i for i in range(1, number_of) if given[i] < largest] or [i for i in range(1, number_of) if given[i] < reach]
        mass, budget = sum([loads[i] for i in candidates]), spare
        for i in candidates:
            more = min(reach - given[i], max(1, budget * loads[i] // mass), spare)
            given[i] = given[i] + more
            spare = spare - more
    return np.array(given)


def scatter_about(stream_key, extent, spread, limit, pieces=(), held_as=jnp.bfloat16):
    factor_of = shard_levels(stream_key, extent, pieces, -0.22, 0.18) if pieces else 1.0
    values = jax.random.normal(stream_key, extent, jnp.float32) * spread * factor_of
    return jnp.minimum(jnp.maximum(values, -limit), limit).astype(held_as)


def setup_inputs(seed: int = 0, part: int = 0) -> dict:
    key_list = jax.random.split(jax.random.key(seed), 7)
    own_keys = jax.random.split(jax.random.fold_in(key_list[6], part), 7)
    tokens = scatter_about(own_keys[0], (TOKENS, D), 1.0, 6.0, ((0, 16),))
    routes_keys = jax.random.split(jax.random.fold_in(own_keys[1], 1), TOKENS // TOK_DEV)
    routes_turns = jax.random.permutation(jax.random.fold_in(own_keys[1], 3), TOKENS // TOK_DEV)
    routes = jax.vmap(lambda own, number: routed_block(jax.random.fold_in(own_keys[1], 2), own, number, TOK_DEV, EXPERTS, TOP, CAP, 2))(routes_keys, routes_turns).reshape((TOKENS, TOP))
    combine_weights = jnp.clip(0.049804688 + 0.9501953 * jax.random.uniform(own_keys[2], (TOKENS, TOP), jnp.float32) ** shard_levels(own_keys[2], (TOKENS, TOP), ((0, 16),), -0.2, 0.2), 0.049804688, 1.0).astype(jnp.bfloat16)
    w_gate = scatter_about(key_list[3], (EXPERTS, D, FF), D ** -0.5, 0.125, ((0, 16),))
    w_up = scatter_about(key_list[4], (EXPERTS, D, FF), D ** -0.5, 0.125, ((0, 16),))
    w_down = scatter_about(key_list[5], (EXPERTS, FF, D), FF ** -0.5, 0.21875, ((0, 16),))
    return {"tokens": tokens, "routes": routes, "combine_weights": combine_weights, "w_gate": w_gate, "w_up": w_up, "w_down": w_down}


def expert_ffn(rows, row_weight, gate_matrix, upward_matrix, down_matrix):
    gate = jnp.dot(rows, gate_matrix, preferred_element_type=jnp.float32)
    upward = jnp.dot(rows, upward_matrix, preferred_element_type=jnp.float32)
    hidden = (jax.nn.silu(gate) * upward).astype(jnp.bfloat16)
    result = jnp.dot(hidden, down_matrix, preferred_element_type=jnp.float32)
    return (result * row_weight.astype(jnp.float32)[:, None]).astype(jnp.bfloat16)


def reference(tokens, routes, combine_weights, w_gate, w_up, w_down):
    pairs = TOKENS * TOP
    flat_routes = routes.reshape(-1)
    flat_weights = combine_weights.reshape(-1)
    room = N_EP * CAP

    def one_expert(total, expert):
        pair_index = jnp.nonzero(flat_routes == expert, size=room, fill_value=pairs)[0].astype(jnp.int32)
        token_index = (pair_index // TOP).astype(jnp.int32)
        rows = jnp.take(tokens, token_index, axis=0, mode="fill", fill_value=0)
        row_weight = jnp.take(flat_weights, pair_index, mode="fill", fill_value=0)
        result = expert_ffn(rows, row_weight, w_gate[expert], w_up[expert], w_down[expert])
        total = total.at[token_index].add(result.astype(jnp.float32), mode="drop")
        return total, None

    start = jnp.zeros((TOKENS, D), jnp.float32)
    total, unused = lax.scan(one_expert, start, jnp.arange(EXPERTS, dtype=jnp.int32))
    return total.astype(jnp.bfloat16)
```

```python
import jax
import jax.numpy as jnp
from jax import lax
from jax.sharding import PartitionSpec as P

AXIS = "ep"
CORES = 2
COLUMNS = 2


def expert_ffn(rows, row_weight, gate_matrix, upward_matrix, down_matrix):
    gate = jnp.dot(rows, gate_matrix, preferred_element_type=jnp.float32)
    upward = jnp.dot(rows, upward_matrix, preferred_element_type=jnp.float32)
    hidden = (jax.nn.silu(gate) * upward).astype(jnp.bfloat16)
    result = jnp.dot(hidden, down_matrix, preferred_element_type=jnp.float32)
    return (result * row_weight.astype(jnp.float32)[:, None]).astype(jnp.bfloat16)


def exchange_plan(tokens, routes, combine_weights, w_gate, w_up, w_down):
    peers = lax.axis_size(AXIS)
    local_tokens, width = tokens.shape
    top_count = routes.shape[1]
    room = min(local_tokens, 3 * local_tokens * top_count // (2 * peers))
    pair_count = local_tokens * top_count
    flat_routes = routes.reshape(-1)
    one_hot = (flat_routes[:, None] == jnp.arange(peers, dtype=jnp.int32)[None, :]).astype(
        jnp.int32
    )
    earlier = jnp.cumsum(one_hot, axis=0) - one_hot
    position = jnp.sum(earlier * one_hot, axis=1)
    slot_index = flat_routes * room + position
    owner = jnp.full((peers * room,), pair_count, jnp.int32)
    owner = owner.at[slot_index].set(jnp.arange(pair_count, dtype=jnp.int32))
    send_rows = jnp.take(tokens, owner // top_count, axis=0, mode="fill", fill_value=0)
    send_rows = send_rows.reshape(peers, room, width)
    send_weight = jnp.take(combine_weights.reshape(-1), owner, mode="fill", fill_value=0)
    send_weight = send_weight.reshape(peers, room)
    arrived, arrived_weight = (
        lax.all_to_all(send_rows, AXIS, split_axis=0, concat_axis=0, tiled=True),
        lax.all_to_all(send_weight, AXIS, split_axis=0, concat_axis=0, tiled=True),
    )
    output = expert_ffn(
        arrived.reshape(peers * room, width),
        arrived_weight.reshape(peers * room),
        w_gate[0],
        w_up[0],
        w_down[0],
    )
    back = lax.all_to_all(
        output.reshape(peers, room, width), AXIS, split_axis=0, concat_axis=0, tiled=True
    )
    per_pair = jnp.take(back.reshape(peers * room, width), slot_index, axis=0)
    summed = jnp.sum(per_pair.reshape(local_tokens, top_count, width).astype(jnp.float32), axis=1)
    return summed.astype(jnp.bfloat16)


def hops(peers):
    step = COLUMNS * CORES
    line = peers // step

    def along(moves):
        return [(a * step + i, b * step + i) for a, b in moves for i in range(step)]

    last, inner = line - 1, line - 2
    return dict(
        core=[(i, i ^ 1) for i in range(peers)],
        column=[(i, i ^ CORES) for i in range(peers)],
        pair=along([(0, 1), (1, 0), (inner, last), (last, inner)]),
        middle=along([(1, inner), (inner, 1)]),
        outward=along([(1, 0), (inner, last)]),
        inward=along([(0, 1), (last, inner)]),
    )


def gather_plan(tokens, routes, combine_weights, w_gate, w_up, w_down):
    peers = lax.axis_size(AXIS)
    local_tokens, width = tokens.shape
    perms = hops(peers)
    step = COLUMNS * CORES
    me = lax.axis_index(AXIS)
    z = me // step
    low = me % step
    is_end = (z == 0) | (z == peers // step - 1)

    def send(value, name):
        return lax.ppermute(value, AXIS, perms[name])

    def add(*terms):
        total = terms[0].astype(jnp.float32)
        for term in terms[1:]:
            total = total + term.astype(jnp.float32)
        return total.astype(jnp.bfloat16)

    experts = jnp.arange(peers, dtype=jnp.int32)
    chosen = routes.T[None, :, :] == experts[:, None, None]
    table = jnp.sum(jnp.where(chosen, combine_weights.T[None].astype(jnp.float32), 0), axis=1)
    table = table.astype(jnp.bfloat16).reshape(peers, 1, local_tokens)
    table = lax.all_to_all(table, AXIS, split_axis=0, concat_axis=0, tiled=True)
    table = table.reshape(peers, local_tokens)
    near = jnp.where(z < 2, 2, 1)
    far = jnp.where(z < 2, 3, 0)
    place = [z, z ^ 1, near, far]

    def weight_of(names):
        parts = []
        for flip_core in (0, 1):
            for k, flip_column in names:
                index = place[k] * step + (low ^ (flip_column * CORES) ^ flip_core)
                parts.append(lax.dynamic_index_in_dim(table, index, 0, keepdims=False))
        return jnp.concatenate(parts)

    own = tokens
    x0 = send(own, "column")
    p1 = send(own, "pair")
    m1 = send(own, "middle")
    x1 = send(p1, "column")
    e2 = send(m1, "outward")
    m2 = send(p1, "middle")
    a2 = jnp.where(is_end, e2, m1)
    x2 = send(a2, "column")
    e3 = send(m2, "outward")
    a3 = jnp.where(is_end, e3, m2)
    x3 = send(a3, "column")

    def run(blocks, names):
        mine = jnp.concatenate(blocks) if len(blocks) > 1 else blocks[0]
        rows = jnp.concatenate([mine, send(mine, "core")])
        result = expert_ffn(rows, weight_of(names), w_gate[0], w_up[0], w_down[0])
        kept, given = jnp.split(result, 2)
        both = add(kept, send(given, "core"))
        return jnp.split(both, len(blocks)) if len(blocks) > 1 else [both]

    (y0,) = run([own], [(0, 0)])
    yx0, y1 = run([x0, p1], [(0, 1), (1, 0)])
    yx1, y2 = run([x1, a2], [(1, 1), (2, 0)])
    yx2, y3 = run([x2, a3], [(2, 1), (3, 0)])
    (yx3,) = run([x3], [(3, 1)])

    s3 = add(y3, send(yx3, "column"))
    t3 = add(s3, send(s3, "inward"))
    s2 = add(y2, send(yx2, "column"))
    u1 = send(t3, "middle")
    t2 = add(s2, send(s2, "inward"))
    s1 = add(y1, send(yx1, "column"), u1)
    v1 = send(s1, "pair")
    v2 = send(t2, "middle")
    return add(y0, send(yx0, "column"), v1, v2)


def solution(mesh):
    peers = mesh.shape[AXIS]
    in_specs = (
        P(("dp", AXIS), None),
        P(("dp", AXIS), None),
        P(("dp", AXIS), None),
        P(AXIS, None, None),
        P(AXIS, None, None),
        P(AXIS, None, None),
    )
    out_specs = P(("dp", AXIS), None)
    line = peers // (COLUMNS * CORES)
    local = gather_plan if line == 4 else exchange_plan
    return jax.shard_map(local, mesh=mesh, in_specs=in_specs, out_specs=out_specs, check_vma=False)
```

```python
import functools

import jax
import jax.numpy as jnp
from jax import lax
from jax.experimental import pallas as pl
from jax.experimental.pallas import tpu as pltpu
from jax.sharding import PartitionSpec as P

AXIS = "ep"
CORES = 2
COLUMNS = 2


def expert_ffn(rows, row_weight, gate_matrix, upward_matrix, down_matrix):
    gate = jnp.dot(rows, gate_matrix, preferred_element_type=jnp.float32)
    upward = jnp.dot(rows, upward_matrix, preferred_element_type=jnp.float32)
    hidden = (jax.nn.silu(gate) * upward).astype(jnp.bfloat16)
    result = jnp.dot(hidden, down_matrix, preferred_element_type=jnp.float32)
    return (result * row_weight.astype(jnp.float32)[:, None]).astype(jnp.bfloat16)


def group_kernel(count, tile, *refs):
    blocks, refs = refs[:count], refs[count:]
    weight_ref, gate_hbm, up_hbm, down_hbm, kept_ref, given_ref = refs[:6]
    rows, gate, up, down, hidden, row_sem, gate_sem, up_sem, down_sem = refs[6:]
    size = blocks[0].shape[0]
    tiles = gate.shape[0]

    def row_copy(k):
        return pltpu.make_async_copy(
            blocks[k], rows.at[pl.ds(k * size, size)], row_sem.at[k]
        )

    def gate_copy(f):
        return pltpu.make_async_copy(
            gate_hbm.at[0, :, pl.ds(f * tile, tile)], gate.at[f], gate_sem.at[f]
        )

    def up_copy(f):
        return pltpu.make_async_copy(
            up_hbm.at[0, :, pl.ds(f * tile, tile)], up.at[f], up_sem.at[f]
        )

    down_copy = pltpu.make_async_copy(down_hbm.at[0], down, down_sem)
    for k in range(count):
        row_copy(k).start()
    for f in range(tiles):
        gate_copy(f).start()
        up_copy(f).start()
    down_copy.start()
    for k in range(count):
        row_copy(k).wait()

    @pl.loop(0, tiles)
    def _(f):
        gate_copy(f).wait()
        up_copy(f).wait()
        g = jnp.dot(rows[...], gate[f], preferred_element_type=jnp.float32)
        u = jnp.dot(rows[...], up[f], preferred_element_type=jnp.float32)
        columns = pl.ds(pl.multiple_of(f * tile, tile), tile)
        hidden[:, columns] = (g / (1 + jnp.exp(-g)) * u).astype(hidden.dtype)

    down_copy.wait()
    half = count // 2 * size

    @pl.loop(0, down.shape[1] // tile)
    def _(n):
        columns = pl.ds(pl.multiple_of(n * tile, tile), tile)
        y = jnp.dot(hidden[...], down[:, columns], preferred_element_type=jnp.float32)
        y = (y * weight_ref[...]).astype(kept_ref.dtype)
        kept_ref[:, columns] = y[:half]
        given_ref[:, columns] = y[half:]


def group_ffn(blocks, row_weight, w_gate, w_up, w_down):
    count = len(blocks)
    size, width = blocks[0].shape
    hidden = w_gate.shape[2]
    tile = 256 if hidden % 256 == 0 and width % 256 == 0 else 128
    tiles = hidden // tile
    total = count * size
    half = jax.ShapeDtypeStruct((total // 2, width), jnp.bfloat16)
    hbm, vmem = pl.BlockSpec(memory_space=pl.ANY), pl.BlockSpec(memory_space=pltpu.VMEM)
    return pl.pallas_call(
        functools.partial(group_kernel, count, tile),
        out_shape=(half, half),
        in_specs=[hbm] * count + [vmem] + [hbm] * 3,
        out_specs=(vmem, vmem),
        scratch_shapes=[
            pltpu.VMEM((total, width), jnp.bfloat16),
            pltpu.VMEM((tiles, width, tile), jnp.bfloat16),
            pltpu.VMEM((tiles, width, tile), jnp.bfloat16),
            pltpu.VMEM((hidden, width), jnp.bfloat16),
            pltpu.VMEM((total, hidden), jnp.bfloat16),
            pltpu.SemaphoreType.DMA((count,)),
            pltpu.SemaphoreType.DMA((tiles,)),
            pltpu.SemaphoreType.DMA((tiles,)),
            pltpu.SemaphoreType.DMA,
        ],
        cost_estimate=pl.CostEstimate(
            flops=6 * total * width * hidden,
            bytes_accessed=6 * width * hidden + 4 * total * width,
            transcendentals=total * hidden,
        ),
        name=f"expert_{count}",
    )(*blocks, row_weight[:, None], w_gate, w_up, w_down)


def exchange_plan(tokens, routes, combine_weights, w_gate, w_up, w_down):
    peers = lax.axis_size(AXIS)
    local_tokens, width = tokens.shape
    top_count = routes.shape[1]
    room = min(local_tokens, 3 * local_tokens * top_count // (2 * peers))
    pair_count = local_tokens * top_count
    flat_routes = routes.reshape(-1)
    one_hot = (flat_routes[:, None] == jnp.arange(peers, dtype=jnp.int32)[None, :]).astype(
        jnp.int32
    )
    earlier = jnp.cumsum(one_hot, axis=0) - one_hot
    position = jnp.sum(earlier * one_hot, axis=1)
    slot_index = flat_routes * room + position
    owner = jnp.full((peers * room,), pair_count, jnp.int32)
    owner = owner.at[slot_index].set(jnp.arange(pair_count, dtype=jnp.int32))
    send_rows = jnp.take(tokens, owner // top_count, axis=0, mode="fill", fill_value=0)
    send_rows = send_rows.reshape(peers, room, width)
    send_weight = jnp.take(combine_weights.reshape(-1), owner, mode="fill", fill_value=0)
    send_weight = send_weight.reshape(peers, room)
    arrived, arrived_weight = (
        lax.all_to_all(send_rows, AXIS, split_axis=0, concat_axis=0, tiled=True),
        lax.all_to_all(send_weight, AXIS, split_axis=0, concat_axis=0, tiled=True),
    )
    output = expert_ffn(
        arrived.reshape(peers * room, width),
        arrived_weight.reshape(peers * room),
        w_gate[0],
        w_up[0],
        w_down[0],
    )
    back = lax.all_to_all(
        output.reshape(peers, room, width), AXIS, split_axis=0, concat_axis=0, tiled=True
    )
    per_pair = jnp.take(back.reshape(peers * room, width), slot_index, axis=0)
    summed = jnp.sum(per_pair.reshape(local_tokens, top_count, width).astype(jnp.float32), axis=1)
    return summed.astype(jnp.bfloat16)


def hops(peers):
    step = COLUMNS * CORES
    line = peers // step

    def along(moves):
        return [(a * step + i, b * step + i) for a, b in moves for i in range(step)]

    last, inner = line - 1, line - 2
    return dict(
        core=[(i, i ^ 1) for i in range(peers)],
        column=[(i, i ^ CORES) for i in range(peers)],
        pair=along([(0, 1), (1, 0), (inner, last), (last, inner)]),
        middle=along([(1, inner), (inner, 1)]),
        outward=along([(1, 0), (inner, last)]),
        inward=along([(0, 1), (last, inner)]),
    )


def gather_plan(tokens, routes, combine_weights, w_gate, w_up, w_down):
    peers = lax.axis_size(AXIS)
    local_tokens, width = tokens.shape
    perms = hops(peers)
    step = COLUMNS * CORES
    me = lax.axis_index(AXIS)
    z = me // step
    low = me % step
    is_end = (z == 0) | (z == peers // step - 1)

    def send(value, name):
        return lax.ppermute(value, AXIS, perms[name])

    def add(*terms):
        total = terms[0].astype(jnp.float32)
        for term in terms[1:]:
            total = total + term.astype(jnp.float32)
        return total.astype(jnp.bfloat16)

    experts = jnp.arange(peers, dtype=jnp.int32)
    chosen = routes.T[None, :, :] == experts[:, None, None]
    table = jnp.sum(jnp.where(chosen, combine_weights.T[None].astype(jnp.float32), 0), axis=1)
    table = table.astype(jnp.bfloat16).reshape(peers, 1, local_tokens)
    table = lax.all_to_all(table, AXIS, split_axis=0, concat_axis=0, tiled=True)
    table = table.reshape(peers, local_tokens)
    near = jnp.where(z < 2, 2, 1)
    far = jnp.where(z < 2, 3, 0)
    place = [z, z ^ 1, near, far]

    def weight_of(names):
        parts = []
        for flip_core in (0, 1):
            for k, flip_column in names:
                index = place[k] * step + (low ^ (flip_column * CORES) ^ flip_core)
                parts.append(lax.dynamic_index_in_dim(table, index, 0, keepdims=False))
        return jnp.concatenate(parts).astype(jnp.float32)

    own = tokens
    x0 = send(own, "column")
    p1 = send(own, "pair")
    m1 = send(own, "middle")
    x1 = send(p1, "column")
    e2 = send(m1, "outward")
    m2 = send(p1, "middle")
    a2 = jnp.where(is_end, e2, m1)
    x2 = send(a2, "column")
    e3 = send(m2, "outward")
    a3 = jnp.where(is_end, e3, m2)
    x3 = send(a3, "column")

    def run(blocks, names):
        others = [send(block, "core") for block in blocks]
        kept, given = group_ffn(blocks + others, weight_of(names), w_gate, w_up, w_down)
        received = send(given, "core")
        return [
            add(kept[k * local_tokens : (k + 1) * local_tokens],
                received[k * local_tokens : (k + 1) * local_tokens])
            for k in range(len(blocks))
        ]

    y0, yx0, y1 = run([own, x0, p1], [(0, 0), (0, 1), (1, 0)])
    yx1, y2 = run([x1, a2], [(1, 1), (2, 0)])
    yx2, y3 = run([x2, a3], [(2, 1), (3, 0)])
    (yx3,) = run([x3], [(3, 1)])

    s3 = add(y3, send(yx3, "column"))
    t3 = add(s3, send(s3, "inward"))
    s2 = add(y2, send(yx2, "column"))
    u1 = send(t3, "middle")
    t2 = add(s2, send(s2, "inward"))
    s1 = add(y1, send(yx1, "column"), u1)
    v1 = send(s1, "pair")
    v2 = send(t2, "middle")
    return add(y0, send(yx0, "column"), v1, v2)


def solution(mesh):
    peers = mesh.shape[AXIS]
    in_specs = (
        P(("dp", AXIS), None),
        P(("dp", AXIS), None),
        P(("dp", AXIS), None),
        P(AXIS, None, None),
        P(AXIS, None, None),
        P(AXIS, None, None),
    )
    out_specs = P(("dp", AXIS), None)
    line = peers // (COLUMNS * CORES)
    local = gather_plan if line == 4 else exchange_plan
    return jax.shard_map(local, mesh=mesh, in_specs=in_specs, out_specs=out_specs, check_vma=False)
```
